32 devices in a mesh: dp: 8 (over z, y), tensor: 4 (over x, core).
Axes of the slice: x: 2, y: 2, z: 4, core: 2. Of those that a mesh axis runs over, the one named last changes fastest.
Arguments:
- layer_input: bfloat16 [1024, 2048], P('dp'), may hold values from -6 to 6
- cotangent: bfloat16 [1024, 2048], P('dp'), may hold values from -6 to 6
- segment_ids: int32 [8, 128], P('dp'), may hold values from 0 to 3, never falling along the last dimension, each value on 1 to 64 neighbouring positions
- routes: int32 [1024, 8], P('dp'), may hold values from 0 to 63, as said below
- attn_gain: float32 [2048], replicated, may hold values from 0.25 to 1.75
- w_query: bfloat16 [2048, 4096], P(None, 'tensor'), may hold values from -0.125 to 0.125
- w_key: bfloat16 [2048, 512], P(None, 'tensor'), may hold values from -0.125 to 0.125
- w_value: bfloat16 [2048, 512], P(None, 'tensor'), may hold values from -0.125 to 0.125
- q_gain: float32 [128], replicated, may hold values from 0.5 to 1.5
- k_gain: float32 [128], replicated, may hold values from 0.5 to 1.5
- w_out: bfloat16 [4096, 2048], P('tensor'), may hold values from -0.375 to 0.375
- ffn_gain: float32 [2048], replicated, may hold values from 0.25 to 1.75
- router: bfloat16 [2048, 64], replicated
- w_gate: bfloat16 [64, 2048, 768], P('dp', None, 'tensor'), may hold values from -0.125 to 0.125
- w_up: bfloat16 [64, 2048, 768], P('dp', None, 'tensor'), may hold values from -0.125 to 0.125
- w_down: bfloat16 [64, 768, 2048], P('dp', 'tensor'), may hold values from -1.25 to 1.25
Outputs:
- layer_out: bfloat16 [1024, 2048], P('dp')
- d_input: float32 [1024, 2048], P('dp')
- grad_attn_gain: float32 [2048], replicated
- grad_query: float32 [2048, 4096], P(None, 'tensor')
- grad_key: float32 [2048, 512], P(None, 'tensor')
- grad_value: float32 [2048, 512], P(None, 'tensor')
- grad_q_gain: float32 [128], replicated
- grad_k_gain: float32 [128], replicated
- grad_out: float32 [4096, 2048], P('tensor')
- grad_ffn_gain: float32 [2048], replicated
- grad_router: float32 [2048, 64], replicated
- grad_gate: float32 [64, 2048, 768], P('dp', None, 'tensor')
- grad_up: float32 [64, 2048, 768], P('dp', None, 'tensor')
- grad_down: float32 [64, 768, 2048], P('dp', 'tensor')
The draws below stay inside these ranges and needn't reach their ends.
Inputs may be any that keep to these rules, and one draw needn't show every extreme that they name: `segment_ids`: in each batch the numbers never fall; each of the 4 sequences has 1 to 64 tokens and one has exactly 64. `routes`: each row names 8 different experts. Among the 128 tokens of one batch no expert is named more than 40 times; in every batch several experts are named exactly 40 times, and some expert is named exactly 40 times in every batch.
All inputs are finite; a program needn't handle non-finite values.
Results may differ from the reference program's by a relative error of at most 0.018.
Values may be sent and summed in bfloat16 or wider, within the bound.
A program may use at most 320 MiB of HBM per device.

```python
import math
import jax
import jax.numpy as jnp
import numpy as np
from jax import lax

D = 2048
Q_HEADS = 32
KV_HEADS = 4
HEAD_DIM = 128
EXP_FF = 768
TOP = 8
EXPERTS = 64
TOK_DEV = 128
SEQS = 4
BATCHES = 8
TOKENS = 1024
CAP = 40
SEQ_MOST = 64
N_TENSOR = 4


def head_gain_draw(key):
    uniform_part = jax.random.uniform(key, (HEAD_DIM,), jnp.float32, 0.0, 1.0)
    values = 0.5 + uniform_part
    return values


def draw_q_gain(key, part):
    return head_gain_draw(jax.random.fold_in(key, 11))


def draw_k_gain(key, part):
    return head_gain_draw(jax.random.fold_in(key, 23))


def draw_router(key, part):
    base_key, scale_key = jax.random.split(jax.random.fold_in(key, 37))
    base_draw = jnp.clip(jax.random.normal(base_key, (D, EXPERTS), jnp.float32), -6.0, 6.0)
    base_draw = base_draw / jnp.sqrt(jnp.float32(D))
    low_log = jnp.log(jnp.float32(0.4))
    high_log = jnp.log(jnp.float32(0.65))
    scales = jnp.exp(low_log + jax.random.uniform(scale_key, (EXPERTS,), jnp.float32, 0.0, 1.0) * (high_log - low_log))
    return (base_draw * scales[None, :]).astype(jnp.bfloat16)


def draw_routes(key, part):
    all_slots = TOK_DEV * TOP
    most_crowded = all_slots // (2 * CAP)
    fewest_crowded = max(1, most_crowded // 2)
    common = min(3, fewest_crowded)
    base_key = jax.random.fold_in(key, 53)
    global_order = jax.random.permutation(jax.random.fold_in(base_key, 1), EXPERTS).astype(jnp.int32)
    index = jnp.arange(EXPERTS, dtype=jnp.int32)
    place_index = jnp.arange(all_slots, dtype=jnp.int32)

    def one_batch(batch_key):
        keys = jax.random.split(batch_key, 5)
        crowded = jax.random.randint(keys[0], (), fewest_crowded, most_crowded + 1, dtype=jnp.int32)
        rest_order = jax.random.permutation(keys[1], EXPERTS - common).astype(jnp.int32)
        labels = jnp.concatenate([global_order[:common], global_order[common:][rest_order]])
        remaining = all_slots - crowded * CAP
        others = EXPERTS - crowded
        base = remaining // others
        leftover = remaining - base * others
        rank = index - crowded
        paired = 2 * (others // 2)
        swing = jax.random.randint(keys[2], (EXPERTS,), -base, base + 1, dtype=jnp.int32)
        sign = 1 - 2 * (rank % 2)
        pair_swing = swing[jnp.clip(rank // 2, 0, EXPERTS - 1)] * sign * (rank < paired).astype(jnp.int32)
        counts = jnp.where(rank < 0, CAP, base + pair_swing + (rank < leftover).astype(jnp.int32))
        bounds = jnp.cumsum(counts).astype(jnp.int32)
        order_index = jnp.searchsorted(bounds, place_index, side='right').astype(jnp.int32)
        expert_ids = labels[order_index].reshape(TOP, TOK_DEV).T
        token_order = jax.random.permutation(keys[3], TOK_DEV).astype(jnp.int32)
        expert_ids = expert_ids[token_order]
        scores = jax.random.randint(keys[4], (TOK_DEV, TOP), 0, 1 << 20, dtype=jnp.int32) * TOP
        scores = scores + jnp.arange(TOP, dtype=jnp.int32)[None, :]
        column_order = jnp.argsort(scores, axis=1)
        return jnp.take_along_axis(expert_ids, column_order, axis=1)
    batch_keys = jax.random.split(jax.random.fold_in(base_key, 2), BATCHES)
    return jax.vmap(one_batch)(batch_keys).reshape(TOKENS, TOP).astype(jnp.int32)


def shard_levels(own_key, shape, cuts, low, high):
    def one(dim, shards_of):
        heights = jax.random.uniform(jax.random.fold_in(jax.random.fold_in(own_key, 6), dim), (shards_of,), jnp.float32, low / len(cuts), high / len(cuts))
        return jnp.repeat(jnp.exp(heights), shape[dim] // shards_of).reshape((-1,) + (1,) * (len(shape) - dim - 1))

    level = one(*cuts[0])
    for cut in cuts[1:]:
        level = level * one(*cut)
    return level


def profile(amount, total, limit, skew):
    loads = [(1 << 20) // math.isqrt(standing ** skew) + 1 for standing in range(2, amount + 1)]
    surplus, holding = total - limit - (amount - 1), [1] * (amount - 1)
    while surplus > 0:
        movable = [i for i in range(amount - 1) if holding[i] < limit]
        whole, left = sum([loads[i] for i in movable]), surplus
        for i in movable:
            more = min(limit - holding[i], max(1, left * loads[i] // whole), surplus)
            holding[i] = holding[i] + more
            surplus = surplus - more
    return np.array([limit] + holding)


def ragged(key, count, total, reach, lean):
    if count == 2:
        one = jax.random.randint(key, (), max(1, total - reach), min(reach, total - 1) + 1)
        return jnp.stack([one, total - one])
    sizes = jnp.asarray(profile(count, total, reach, lean), jnp.int32)
    twos = (count - 1) // 2
    giver, taker = sizes[1:1 + 2 * twos:2], sizes[2:2 + 2 * twos:2]
    room = jnp.minimum(giver - 1, reach - taker)
    shifted = jax.random.randint(jax.random.fold_in(key, 1), (twos,), 0, 1 << 20) % (room + 1)
    sizes = sizes.at[1:1 + 2 * twos:2].set(giver - shifted).at[2:2 + 2 * twos:2].set(taker + shifted)
    return sizes[jax.random.permutation(jax.random.fold_in(key, 2), count)]


def noise(own_key, dims, width, reach, shards=(), held_as=jnp.bfloat16):
    result = width * jax.random.normal(own_key, dims, jnp.float32)
    if shards:
        result = result * shard_levels(own_key, dims, shards, -0.22, 0.18)
    return jnp.clip(result, -reach, reach).astype(held_as)


def setup_inputs(seed: int = 0) -> dict:
    splits = jax.random.split(jax.random.key(seed), 17)
    layer_input = noise(splits[0], (TOKENS, D), 1.0, 6.0, ((0, 8),))
    cotangent = noise(splits[1], (TOKENS, D), 1.0, 6.0, ((0, 8),))
    segment_ids = jax.vmap(lambda own: jnp.searchsorted(jnp.cumsum(ragged(own, SEQS, TOK_DEV, SEQ_MOST, 2)), jnp.arange(TOK_DEV), side="right"))(jax.random.split(splits[2], BATCHES)).reshape((BATCHES, TOK_DEV)).astype(jnp.int32)
    routes = draw_routes(jax.random.fold_in(splits[16], 71), 0)
    attn_gain = jnp.clip(1.0 + 0.15 * jax.random.normal(splits[4], (D,), jnp.float32), 0.25, 1.75)
    w_query = noise(splits[5], (D, Q_HEADS * HEAD_DIM), D ** -0.5, 0.125, ((1, 4),))
    w_key = noise(splits[6], (D, KV_HEADS * HEAD_DIM), D ** -0.5, 0.125, ((1, 4),))
    w_value = noise(splits[7], (D, KV_HEADS * HEAD_DIM), D ** -0.5, 0.125, ((1, 4),))
    q_gain = draw_q_gain(jax.random.fold_in(splits[16], 71), 0)
    k_gain = draw_k_gain(jax.random.fold_in(splits[16], 71), 0)
    w_out = noise(splits[10], (Q_HEADS * HEAD_DIM, D), (Q_HEADS * HEAD_DIM // 16) ** -0.5, 0.375, ((0, 4),))
    ffn_gain = jnp.clip(1.0 + 0.15 * jax.random.normal(splits[11], (D,), jnp.float32), 0.25, 1.75)
    router = draw_router(jax.random.fold_in(splits[16], 71), 0)
    w_gate = noise(splits[13], (EXPERTS, D, EXP_FF), D ** -0.5, 0.125, ((0, 8), (2, 4)))
    w_up = noise(splits[14], (EXPERTS, D, EXP_FF), D ** -0.5, 0.125, ((0, 8), (2, 4)))
    w_down = noise(splits[15], (EXPERTS, EXP_FF, D), (EXP_FF // 32) ** -0.5, 1.25, ((0, 8), (1, 4)))
    return dict(layer_input=layer_input, cotangent=cotangent, segment_ids=segment_ids, routes=routes, attn_gain=attn_gain, w_query=w_query, w_key=w_key, w_value=w_value, q_gain=q_gain, k_gain=k_gain, w_out=w_out, ffn_gain=ffn_gain, router=router, w_gate=w_gate, w_up=w_up, w_down=w_down)


EPSILON = 1e-06
ROPE_BASE = 1000000.0

def rms_scale(values, gain_vec):
    return values * lax.rsqrt(lax.optimization_barrier(jnp.mean(values * values, axis=-1, keepdims=True)) + EPSILON) * gain_vec

def rounded(values):
    return lax.optimization_barrier(values.astype(jnp.bfloat16)).astype(jnp.float32)

def seq_positions(segments):
    position_index = jnp.arange(segments.shape[0], dtype=jnp.int32)
    begins = jnp.concatenate([jnp.ones((1,), dtype=jnp.bool_), segments[1:] != segments[:-1]])
    first_index = lax.cummax(jnp.where(begins, position_index, jnp.zeros_like(position_index)), axis=0)
    return position_index - first_index

def rope_tables(positions, head_dim):
    half_dim = head_dim // 2
    exponent = jnp.arange(half_dim, dtype=jnp.float32) * (2.0 / head_dim)
    frequency = jnp.exp(-exponent * jnp.log(jnp.float32(ROPE_BASE)))
    angle_table = positions.astype(jnp.float32)[:, None] * frequency[None, :]
    angle_table = jnp.concatenate([angle_table, angle_table], axis=1)
    return (jnp.cos(angle_table), jnp.sin(angle_table))

def head_prep(raw_proj, gain_vec, cosine_table, sine_table):
    row_count = raw_proj.shape[0]
    head_dim = gain_vec.shape[0]
    split_heads = rms_scale(raw_proj.reshape(row_count, -1, head_dim), gain_vec)
    half_dim = head_dim // 2
    turned = jnp.concatenate([-split_heads[..., half_dim:], split_heads[..., :half_dim]], axis=-1)
    rotated = split_heads * cosine_table[:, None, :] + turned * sine_table[:, None, :]
    return rotated.reshape(row_count, -1)

def gate_weights(logits, routes):
    route_marks = (routes[:, :, None] == jnp.arange(logits.shape[1], dtype=jnp.int32)[None, None, :]).astype(logits.dtype)
    chosen = lax.optimization_barrier(jnp.sum(logits[:, None, :] * route_marks, axis=-1))
    return jax.nn.softmax(chosen, axis=-1)

def slot_tables(routes, experts_here, groups, capacity):
    row_count, top_count = routes.shape
    flat_routes = routes.reshape(-1)
    route_marks = (flat_routes[:, None] == jnp.arange(experts_here * groups, dtype=jnp.int32)[None, :]).astype(jnp.int32)
    earlier = jnp.cumsum(route_marks, axis=0) - route_marks
    placing = lax.optimization_barrier(jnp.sum(earlier * route_marks, axis=1))
    holder = flat_routes // experts_here
    local_id = flat_routes % experts_here
    buffer_slot = (local_id * groups + holder) * capacity + placing
    owner_slot = jnp.full((experts_here * groups * capacity,), row_count * top_count, dtype=jnp.int32)
    owner_slot = owner_slot.at[buffer_slot].set(jnp.arange(row_count * top_count, dtype=jnp.int32))
    return (buffer_slot, owner_slot)

def masked_scores(query_block, key_heads, segments, first_row):
    block_rows = query_block.shape[0]
    scores = jnp.einsum('qhgd,shd->hgqs', query_block.astype(jnp.float32), key_heads.astype(jnp.float32))
    scores = scores * query_block.shape[-1] ** (-0.5)
    query_index = first_row + jnp.arange(block_rows, dtype=jnp.int32)
    key_index = jnp.arange(key_heads.shape[0], dtype=jnp.int32)
    query_segs = segments[first_row:first_row + block_rows]
    allowed = (query_segs[:, None] == segments[None, :]) & (query_index[:, None] >= key_index[None, :])
    return jnp.where(allowed[None, None], scores, -jnp.inf)

def attend(query_rot, key_rot, value_rot, segments, kv_count, head_dim):
    row_count = query_rot.shape[0]
    query_heads = query_rot.reshape(row_count, kv_count, -1, head_dim)
    key_heads = key_rot.reshape(row_count, kv_count, head_dim)
    value_heads = value_rot.reshape(row_count, kv_count, head_dim)
    block_rows = min(512, row_count)
    out_list = []
    lse_list = []
    for first_row in range(0, row_count, block_rows):
        scores = masked_scores(query_heads[first_row:first_row + block_rows], key_heads, segments, first_row)
        highest = lax.optimization_barrier(jnp.max(scores, axis=-1, keepdims=True))
        exponent = jnp.exp(scores - highest)
        denominator = lax.optimization_barrier(jnp.sum(exponent, axis=-1, keepdims=True))
        probs_bf = rounded(exponent / denominator)
        lse_list.append(highest[..., 0] + jnp.log(denominator[..., 0]))
        head_mix = jnp.einsum('hgqs,shd->qhgd', probs_bf, value_heads.astype(jnp.float32))
        out_list.append(head_mix.astype(jnp.bfloat16).reshape(block_rows, -1))
    return (jnp.concatenate(out_list, axis=0), jnp.concatenate(lse_list, axis=-1))

def attend_back(query_rot, key_rot, value_rot, segments, log_total, grad_heads, kv_count, head_dim):
    row_count = query_rot.shape[0]
    query_heads = query_rot.reshape(row_count, kv_count, -1, head_dim)
    key_heads = key_rot.reshape(row_count, kv_count, head_dim)
    value_heads = value_rot.reshape(row_count, kv_count, head_dim)
    block_rows = min(512, row_count)
    score_scale = head_dim ** (-0.5)
    d_keys = jnp.zeros((row_count, kv_count, head_dim), jnp.float32)
    d_values = jnp.zeros((row_count, kv_count, head_dim), jnp.float32)
    dq_list = []
    for first_row in range(0, row_count, block_rows):
        query_block = query_heads[first_row:first_row + block_rows]
        scores = masked_scores(query_block, key_heads, segments, first_row)
        probabilities = jnp.exp(scores - log_total[..., first_row:first_row + block_rows, None])
        grad_block = grad_heads[first_row:first_row + block_rows].reshape(block_rows, kv_count, -1, head_dim).astype(jnp.float32)
        d_values = d_values + jnp.einsum('hgqs,qhgd->shd', rounded(probabilities), grad_block)
        d_prob = jnp.einsum('qhgd,shd->hgqs', grad_block, value_heads.astype(jnp.float32))
        row_delta = lax.optimization_barrier(jnp.sum(probabilities * d_prob, axis=-1, keepdims=True))
        d_score = rounded(probabilities * (d_prob - row_delta) * score_scale)
        dq_list.append(jnp.einsum('hgqs,shd->qhgd', d_score, key_heads.astype(jnp.float32)).reshape(block_rows, -1))
        d_keys = d_keys + jnp.einsum('hgqs,qhgd->shd', d_score, query_block.astype(jnp.float32))
    return (jnp.concatenate(dq_list, axis=0), d_keys.reshape(row_count, -1), d_values.reshape(row_count, -1))

def attention_part(x_rows, segments, attn_gain, w_query, w_key, w_value, q_gain, k_gain, w_out, ffn_gain, router):
    x_float = x_rows.astype(jnp.float32)
    cosine_table, sine_table = rope_tables(seq_positions(segments), HEAD_DIM)
    normed1 = rms_scale(x_float, attn_gain).astype(jnp.bfloat16)
    query_raw = jnp.dot(normed1, w_query, preferred_element_type=jnp.float32)
    key_raw = jnp.dot(normed1, w_key, preferred_element_type=jnp.float32)
    value_rot = jnp.dot(normed1, w_value, preferred_element_type=jnp.float32).astype(jnp.bfloat16)
    query_rot = head_prep(query_raw, q_gain, cosine_table, sine_table).astype(jnp.bfloat16)
    key_rot = head_prep(key_raw, k_gain, cosine_table, sine_table).astype(jnp.bfloat16)
    attn_mixed, log_total = attend(query_rot, key_rot, value_rot, segments, KV_HEADS, HEAD_DIM)
    residual = x_float + jnp.dot(attn_mixed, w_out, preferred_element_type=jnp.float32)
    normed2 = rms_scale(residual, ffn_gain).astype(jnp.bfloat16)
    logits = jnp.dot(normed2, router, preferred_element_type=jnp.float32)
    return (x_float, cosine_table, sine_table, normed1, query_raw, key_raw, query_rot, key_rot, value_rot, attn_mixed, log_total, residual, normed2, logits)

def expert_forward(inputs, gate_w, up_w, down_w):
    gate_pre = jnp.dot(inputs, gate_w, preferred_element_type=jnp.float32)
    up_pre = jnp.dot(inputs, up_w, preferred_element_type=jnp.float32)
    activation = (gate_pre * jax.nn.sigmoid(gate_pre) * up_pre).astype(jnp.bfloat16)
    slot_count = inputs.shape[0]
    pieces = jnp.einsum('rjf,jfd->rjd', activation.reshape(slot_count, N_TENSOR, -1).astype(jnp.float32), down_w.reshape(N_TENSOR, -1, down_w.shape[1]).astype(jnp.float32))
    return (gate_pre, up_pre, activation, lax.optimization_barrier(jnp.sum(rounded(pieces), axis=1)))

def reference(layer_input, cotangent, segment_ids, routes, attn_gain, w_query, w_key, w_value, q_gain, k_gain, w_out, ffn_gain, router, w_gate, w_up, w_down):
    weight_list = (attn_gain, w_query, w_key, w_value, q_gain, k_gain, w_out, ffn_gain, router)
    x_batches = layer_input.reshape(BATCHES, TOK_DEV, D)
    cot_batches = cotangent.reshape(BATCHES, TOK_DEV, D)
    route_batches = routes.reshape(BATCHES, TOK_DEV, TOP)

    def forward_batch(packed):
        x_rows, segments, route_rows = packed
        pieces = attention_part(x_rows, segments, *weight_list)
        weights = gate_weights(pieces[13], route_rows)
        owner_slot = slot_tables(route_rows, EXPERTS, 1, CAP)[1]
        return (pieces[11], pieces[12], weights, owner_slot)
    residual, normed2, weights, owners = lax.map(forward_batch, (x_batches, segment_ids, route_batches))
    flat_count = TOKENS * TOP
    owners = owners.reshape(BATCHES, EXPERTS, CAP)
    batch_base = (jnp.arange(BATCHES, dtype=jnp.int32) * (TOK_DEV * TOP))[:, None, None]
    global_slots = jnp.where(owners < TOK_DEV * TOP, owners + batch_base, flat_count)
    global_slots = jnp.transpose(global_slots, (1, 0, 2)).reshape(EXPERTS, BATCHES * CAP)
    normed_pad = jnp.concatenate([normed2.reshape(TOKENS, D), jnp.zeros((1, D), jnp.bfloat16)], axis=0)
    weight_pad = jnp.concatenate([weights.reshape(-1), jnp.zeros((1,), jnp.float32)])
    cot_pad = jnp.concatenate([cotangent, jnp.zeros((1, D), jnp.bfloat16)], axis=0)

    def expert_fwd(moe_accum, packed):
        gate_w, up_w, down_w, slot_ids = packed
        token_ids = slot_ids // TOP
        full_out = expert_forward(normed_pad[token_ids], gate_w, up_w, down_w)[3]
        return (moe_accum.at[token_ids].add(weight_pad[slot_ids][:, None] * full_out), None)
    moe_total, _ = lax.scan(expert_fwd, jnp.zeros((TOKENS + 1, D), jnp.float32), (w_gate, w_up, w_down, global_slots))
    layer_out = (residual.reshape(TOKENS, D) + moe_total[:TOKENS]).astype(jnp.bfloat16)

    def expert_back(held_sums, packed):
        dw_accum, dn_accum = held_sums
        gate_w, up_w, down_w, slot_ids = packed
        token_ids = slot_ids // TOP
        inputs = normed_pad[token_ids]
        gate_pre, up_pre, activation, full_out = expert_forward(inputs, gate_w, up_w, down_w)
        cot_rows = cot_pad[token_ids].astype(jnp.float32)
        dw_accum = dw_accum.at[slot_ids].add(lax.optimization_barrier(jnp.sum(cot_rows * full_out, axis=1)))
        slot_grad = (weight_pad[slot_ids][:, None] * cot_rows).astype(jnp.bfloat16)
        d_act = jnp.dot(slot_grad, down_w.T, preferred_element_type=jnp.float32)
        sigmoid_g = jax.nn.sigmoid(gate_pre)
        d_gate = (d_act * up_pre * sigmoid_g * (1.0 + gate_pre * (1.0 - sigmoid_g))).astype(jnp.bfloat16)
        d_up = (d_act * (gate_pre * sigmoid_g)).astype(jnp.bfloat16)
        grad_down_e = jnp.dot(activation.T, slot_grad, preferred_element_type=jnp.float32)
        grad_gate_e = jnp.dot(inputs.T, d_gate, preferred_element_type=jnp.float32)
        grad_up_e = jnp.dot(inputs.T, d_up, preferred_element_type=jnp.float32)
        slot_count = inputs.shape[0]
        quarter = jnp.einsum('rjf,djf->rjd', d_gate.reshape(slot_count, N_TENSOR, -1).astype(jnp.float32), gate_w.reshape(D, N_TENSOR, -1).astype(jnp.float32))
        quarter = quarter + jnp.einsum('rjf,djf->rjd', d_up.reshape(slot_count, N_TENSOR, -1).astype(jnp.float32), up_w.reshape(D, N_TENSOR, -1).astype(jnp.float32))
        dn_accum = dn_accum.at[token_ids].add(lax.optimization_barrier(jnp.sum(rounded(quarter), axis=1)))
        return ((dw_accum, dn_accum), (grad_gate_e, grad_up_e, grad_down_e))
    init_back = (jnp.zeros((flat_count + 1,), jnp.float32), jnp.zeros((TOKENS + 1, D), jnp.float32))
    (dw_flat, dn_moe), expert_grads = lax.scan(expert_back, init_back, (w_gate, w_up, w_down, global_slots))
    d_weights = dw_flat[:flat_count].reshape(BATCHES, TOK_DEV, TOP)
    d_norm2_moe = dn_moe[:TOKENS].reshape(BATCHES, TOK_DEV, D)

    def backward_batch(held_sums, packed):
        x_rows, segments, route_rows, cot_rows, dw_rows, dn_rows = packed
        x_float, cosine_table, sine_table, normed1, query_raw, key_raw, query_rot, key_rot, value_rot, attn_mixed, log_total, residual_b, normed2_b, logits = attention_part(x_rows, segments, *weight_list)
        gate_back = jax.vjp(lambda logit_in: gate_weights(logit_in, route_rows), logits)[1]
        d_logits = gate_back(dw_rows)[0].astype(jnp.bfloat16)
        grad_router = jnp.dot(normed2_b.T, d_logits, preferred_element_type=jnp.float32)
        d_norm2 = dn_rows + jnp.dot(d_logits, router.T, preferred_element_type=jnp.float32)
        norm2_back = jax.vjp(rms_scale, residual_b, ffn_gain)[1]
        d_resid_norm, grad_ffn_gain = norm2_back(d_norm2)
        d_resid = cot_rows.astype(jnp.float32) + d_resid_norm
        d_resid_bf = d_resid.astype(jnp.bfloat16)
        grad_out_w = jnp.dot(attn_mixed.T, d_resid_bf, preferred_element_type=jnp.float32)
        d_attn = jnp.dot(d_resid_bf, w_out.T, preferred_element_type=jnp.float32).astype(jnp.bfloat16)
        d_qrot, d_krot, d_vals = attend_back(query_rot, key_rot, value_rot, segments, log_total, d_attn, KV_HEADS, HEAD_DIM)
        q_back = jax.vjp(lambda raw_in, gain_in: head_prep(raw_in, gain_in, cosine_table, sine_table), query_raw, q_gain)[1]
        d_qraw, grad_qgain = q_back(d_qrot)
        k_back = jax.vjp(lambda raw_in, gain_in: head_prep(raw_in, gain_in, cosine_table, sine_table), key_raw, k_gain)[1]
        d_kraw, grad_kgain = k_back(d_krot)
        dq_bf = d_qraw.astype(jnp.bfloat16)
        dk_bf = d_kraw.astype(jnp.bfloat16)
        dv_bf = d_vals.astype(jnp.bfloat16)
        grad_query = jnp.dot(normed1.T, dq_bf, preferred_element_type=jnp.float32)
        grad_key = jnp.dot(normed1.T, dk_bf, preferred_element_type=jnp.float32)
        grad_value = jnp.dot(normed1.T, dv_bf, preferred_element_type=jnp.float32)
        d_norm1 = jnp.dot(dq_bf, w_query.T, preferred_element_type=jnp.float32)
        d_norm1 = d_norm1 + jnp.dot(dk_bf, w_key.T, preferred_element_type=jnp.float32)
        d_norm1 = d_norm1 + jnp.dot(dv_bf, w_value.T, preferred_element_type=jnp.float32)
        norm1_back = jax.vjp(rms_scale, x_float, attn_gain)[1]
        d_x_norm, grad_attn_gain = norm1_back(d_norm1)
        new_grads = (grad_attn_gain, grad_query, grad_key, grad_value, grad_qgain, grad_kgain, grad_out_w, grad_ffn_gain, grad_router)
        return (tuple((held_sum + new_sum for held_sum, new_sum in zip(held_sums, new_grads))), d_resid + d_x_norm)
    init_grads = tuple((jnp.zeros(weight_item.shape, jnp.float32) for weight_item in weight_list))
    grad_sums, d_input = lax.scan(backward_batch, init_grads, (x_batches, segment_ids, route_batches, cot_batches, d_weights, d_norm2_moe))
    return (layer_out, d_input.reshape(TOKENS, D), grad_sums[0], grad_sums[1], grad_sums[2], grad_sums[3], grad_sums[4], grad_sums[5], grad_sums[6], grad_sums[7], grad_sums[8], expert_grads[0], expert_grads[1], expert_grads[2])
```

```python
import jax
import jax.numpy as jnp
from jax import lax
from jax.sharding import PartitionSpec as P

CAP = 40
EPSILON = 1e-06
ROPE_BASE = 1000000.0
BF = jnp.bfloat16
F32 = jnp.float32


def rms_scale(values, gain_vec):
    return (
        values * lax.rsqrt(jnp.mean(values * values, axis=-1, keepdims=True) + EPSILON) * gain_vec
    )


def seq_positions(segments):
    index = jnp.arange(segments.shape[0], dtype=jnp.int32)
    before = jnp.sum((segments[None, :] < segments[:, None]).astype(jnp.int32), axis=1)
    return index - before


def rope_tables(positions, head_dim):
    half_dim = head_dim // 2
    exponent = jnp.arange(half_dim, dtype=F32) * (2.0 / head_dim)
    frequency = jnp.exp(-exponent * jnp.log(F32(ROPE_BASE)))
    angle_table = positions.astype(F32)[:, None] * frequency[None, :]
    angle_table = jnp.concatenate([angle_table, angle_table], axis=1)
    return (jnp.cos(angle_table), jnp.sin(angle_table))


def head_prep(raw_proj, gain_vec, cosine_table, sine_table):
    row_count = raw_proj.shape[0]
    head_dim = gain_vec.shape[0]
    split_heads = rms_scale(raw_proj.reshape(row_count, -1, head_dim), gain_vec)
    half_dim = head_dim // 2
    turned = jnp.concatenate([-split_heads[..., half_dim:], split_heads[..., :half_dim]], axis=-1)
    rotated = split_heads * cosine_table[:, None, :] + turned * sine_table[:, None, :]
    return rotated.reshape(row_count, -1)


def masked_scores(query_heads, key_heads, segments):
    rows = query_heads.shape[0]
    scores = jnp.einsum("qhgd,shd->hgqs", query_heads, key_heads, preferred_element_type=F32)
    scores = scores * query_heads.shape[-1] ** (-0.5)
    index = jnp.arange(rows, dtype=jnp.int32)
    allowed = (segments[:, None] == segments[None, :]) & (index[:, None] >= index[None, :])
    return jnp.where(allowed[None, None], scores, -jnp.inf)


def attend(query_rot, key_rot, value_rot, segments, kv_count, head_dim):
    rows = query_rot.shape[0]
    query_heads = query_rot.reshape(rows, kv_count, -1, head_dim)
    key_heads = key_rot.reshape(rows, kv_count, head_dim)
    value_heads = value_rot.reshape(rows, kv_count, head_dim)
    scores = masked_scores(query_heads, key_heads, segments)
    highest = jnp.max(scores, axis=-1, keepdims=True)
    exponent = jnp.exp(scores - highest)
    denominator = jnp.sum(exponent, axis=-1, keepdims=True)
    probs_bf = (exponent / denominator).astype(BF)
    lse = highest[..., 0] + jnp.log(denominator[..., 0])
    mixed = jnp.einsum("hgqs,shd->qhgd", probs_bf, value_heads, preferred_element_type=F32)
    return (mixed.astype(BF).reshape(rows, -1), lse)


def attend_back(query_rot, key_rot, value_rot, segments, lse, grad_heads, kv_count, head_dim):
    rows = query_rot.shape[0]
    query_heads = query_rot.reshape(rows, kv_count, -1, head_dim)
    key_heads = key_rot.reshape(rows, kv_count, head_dim)
    value_heads = value_rot.reshape(rows, kv_count, head_dim)
    scores = masked_scores(query_heads, key_heads, segments)
    probs = jnp.exp(scores - lse[..., None])
    grad_block = grad_heads.reshape(rows, kv_count, -1, head_dim)
    d_values = jnp.einsum(
        "hgqs,qhgd->shd", probs.astype(BF), grad_block, preferred_element_type=F32
    )
    d_prob = jnp.einsum("qhgd,shd->hgqs", grad_block, value_heads, preferred_element_type=F32)
    row_delta = jnp.sum(probs * d_prob, axis=-1, keepdims=True)
    d_score = (probs * (d_prob - row_delta) * head_dim ** (-0.5)).astype(BF)
    d_query = jnp.einsum("hgqs,shd->qhgd", d_score, key_heads, preferred_element_type=F32)
    d_keys = jnp.einsum("hgqs,qhgd->shd", d_score, query_heads, preferred_element_type=F32)
    return (d_query.reshape(rows, -1), d_keys.reshape(rows, -1), d_values.reshape(rows, -1))


def make_device_fn(mesh):
    n_dp = mesh.shape["dp"]
    n_tp = mesh.shape["tensor"]

    def rot(x, step):
        return lax.ppermute(x, "dp", [(i, (i + step) % n_dp) for i in range(n_dp)])

    def flip(x, mask):
        return lax.ppermute(x, "tensor", [(i, i ^ mask) for i in range(n_tp)])

    def relative(quarters):
        own = lax.axis_index("tensor")
        for bit in (1, 2):
            on = (own & bit) != 0
            quarters = [
                jnp.where(on, quarters[q ^ bit], quarters[q]) for q in range(n_tp)
            ]
        return quarters

    def split_relative(x):
        return relative(jnp.split(x, n_tp, axis=0))

    def over_tensor(x):
        across = flip(x, 2)
        return [x, flip(x, 1), across, flip(across, 1)]

    def gather_tokens(x):
        blocks = []
        for step in range(n_dp):
            blocks.extend(over_tensor(x if step == 0 else rot(x, step)))
        return jnp.concatenate(blocks, axis=0)

    def gather_batches(x):
        return jnp.concatenate([x] + [rot(x, s) for s in range(1, n_dp)], axis=0)

    def add_up(a, b, kind):
        return (a.astype(F32) + b.astype(F32)).astype(kind)

    def reduce_tensor(parts, kind, last):
        low = add_up(parts[0], flip(parts[1], 1), kind)
        high = add_up(parts[2], flip(parts[3], 1), kind)
        return add_up(low, flip(high, 2), last)

    def reduce_tokens(x, rows):
        grid = x.reshape(n_dp, n_tp, rows, x.shape[1])
        total = None
        for step in list(range(1, n_dp)) + [0]:
            part = reduce_tensor([grid[step, m] for m in range(n_tp)], BF, BF)
            part = part if step == 0 else rot(part, n_dp - step)
            total = part.astype(F32) if total is None else total + part.astype(F32)
        return total

    def sum_all(x):
        total = x
        for step in range(1, n_dp):
            total = total + rot(x, step)
        return sum(over_tensor(total)[1:], total)

    def on_device(
        layer_input,
        cotangent,
        segment_ids,
        routes,
        attn_gain,
        w_query,
        w_key,
        w_value,
        q_gain,
        k_gain,
        w_out,
        ffn_gain,
        router,
        w_gate,
        w_up,
        w_down,
    ):
        segments = segment_ids[0]
        row_count, width = layer_input.shape
        own_rows = row_count // n_tp
        head_dim = q_gain.shape[0]
        kv_here = w_key.shape[1] // head_dim
        experts_here = w_gate.shape[0]
        experts = router.shape[1]
        tokens = n_dp * row_count
        slots = n_dp * CAP
        tensor_at = lax.axis_index("tensor")
        first_expert = lax.axis_index("dp") * experts_here
        first_row = tensor_at * own_rows

        def own(x):
            return lax.dynamic_slice_in_dim(x, first_row, own_rows, axis=0)

        route_rows = jnp.concatenate(split_relative(routes), axis=0)
        routes_all = gather_batches(route_rows.T.reshape(1, -1, row_count))
        routes_all = jnp.transpose(routes_all, (0, 2, 1)).reshape(tokens, -1)
        cot_all = gather_tokens(own(cotangent))

        cosine_table, sine_table = rope_tables(seq_positions(segments), head_dim)
        x_float = layer_input.astype(F32)
        normed1 = rms_scale(x_float, attn_gain).astype(BF)
        query_raw = jnp.dot(normed1, w_query, preferred_element_type=F32)
        key_raw = jnp.dot(normed1, w_key, preferred_element_type=F32)
        value_rot = jnp.dot(normed1, w_value, preferred_element_type=F32).astype(BF)
        query_rot = head_prep(query_raw, q_gain, cosine_table, sine_table).astype(BF)
        key_rot = head_prep(key_raw, k_gain, cosine_table, sine_table).astype(BF)
        attn_mixed, lse = attend(query_rot, key_rot, value_rot, segments, kv_here, head_dim)
        partial_attn = jnp.dot(attn_mixed, w_out, preferred_element_type=F32)
        x_own = own(layer_input).astype(F32)
        residual = x_own + reduce_tensor(split_relative(partial_attn), F32, F32)
        normed2 = rms_scale(residual, ffn_gain).astype(BF)

        normed_all = gather_tokens(normed2)
        attn_all = gather_batches(jnp.concatenate(split_relative(attn_mixed), axis=0))

        def dense_weights(rows, chosen):
            logits = jnp.dot(rows, router, preferred_element_type=F32)
            marks = jnp.any(
                chosen[:, :, None] == jnp.arange(experts, dtype=jnp.int32)[None, None, :], axis=1
            )
            shown = jnp.where(marks, logits, -jnp.inf)
            power = jnp.exp(shown - jnp.max(shown, axis=-1, keepdims=True))
            return power / jnp.sum(power, axis=-1, keepdims=True)

        weights_all = dense_weights(normed_all, routes_all)
        weights_here = lax.dynamic_slice_in_dim(weights_all.T, first_expert, experts_here, axis=0)
        names = first_expert + jnp.arange(experts_here, dtype=jnp.int32)
        marks = jnp.any(routes_all.T[None] == names[:, None, None], axis=1)
        index = jnp.arange(row_count, dtype=jnp.int32)
        earlier = (index[:, None] < index[None, :]).astype(BF)
        grouped = marks.astype(BF).reshape(experts_here, n_dp, row_count)
        place = jnp.einsum("ebt,tu->ebu", grouped, earlier, preferred_element_type=F32)
        counts = jnp.sum(grouped.astype(F32), axis=2)
        batch_at = jnp.arange(n_dp)
        begins = jnp.sum(
            jnp.where(batch_at[:, None] > batch_at[None, :], counts[:, None, :], 0.0), axis=2
        )
        place = (place + begins[:, :, None]).astype(jnp.int32).reshape(experts_here, tokens)
        place = jnp.where(marks, place, -1)
        picks = place[:, None, :] == jnp.arange(slots, dtype=jnp.int32)[None, :, None]
        one_hot = picks.astype(BF).reshape(experts_here * slots, tokens)

        def to_slots(rows):
            packed = jnp.dot(one_hot, rows, preferred_element_type=F32).astype(BF)
            return packed.reshape(experts_here, slots, width)

        def to_tokens(packed):
            packed = packed.reshape(experts_here * slots, width)
            return lax.dot_general(
                one_hot, packed, (((0,), (0,)), ((), ())), preferred_element_type=F32
            ).astype(BF)

        slot_weight = jnp.sum(jnp.where(picks, weights_here[:, None, :], 0.0), axis=2)

        cot_in = to_slots(cot_all)
        raw_act = jnp.einsum("erd,efd->erf", cot_in, w_down, preferred_element_type=F32)
        expert_in = to_slots(normed_all)
        gate_pre = jnp.einsum("erd,edf->erf", expert_in, w_gate, preferred_element_type=F32)
        up_pre = jnp.einsum("erd,edf->erf", expert_in, w_up, preferred_element_type=F32)
        sigmoid_g = jax.nn.sigmoid(gate_pre)
        silu_g = gate_pre * sigmoid_g
        activation = (silu_g * up_pre).astype(BF).astype(F32)
        slot_dw = jnp.sum(activation * raw_act, axis=2)
        weighted = (activation * slot_weight[:, :, None]).astype(BF)
        d_act = raw_act * slot_weight[:, :, None]
        d_gate = (d_act * up_pre * sigmoid_g * (1.0 + gate_pre * (1.0 - sigmoid_g))).astype(BF)
        d_up = (d_act * silu_g).astype(BF)
        d_in = jnp.einsum("erf,edf->erd", d_gate, w_gate, preferred_element_type=F32)
        d_in = (
            d_in + jnp.einsum("erf,edf->erd", d_up, w_up, preferred_element_type=F32)
        ).astype(BF)
        d_weights = jnp.sum(jnp.where(picks, slot_dw[:, :, None], 0.0), axis=1)
        d_weights = lax.dynamic_update_slice(
            jnp.zeros((-(-experts // 128) * 128, tokens), F32), d_weights, (first_expert, 0)
        )
        back = jnp.concatenate([to_tokens(d_in), d_weights.T.astype(BF)], axis=1)
        back = reduce_tokens(back, own_rows)

        expert_out = jnp.einsum(
            "erf,efd->erd", weighted, w_down, preferred_element_type=F32
        ).astype(BF)
        moe = reduce_tokens(to_tokens(expert_out), own_rows)
        layer_out = (residual + moe).astype(BF)
        layer_out = jnp.concatenate(relative(over_tensor(layer_out)), axis=0)
        grad_down = jnp.einsum("erf,erd->efd", weighted, cot_in, preferred_element_type=F32)
        grad_gate = jnp.einsum("erd,erf->edf", expert_in, d_gate, preferred_element_type=F32)
        grad_up = jnp.einsum("erd,erf->edf", expert_in, d_up, preferred_element_type=F32)

        weights_own = dense_weights(normed2, own(routes))
        dw_own = back[:, width : width + experts]
        d_logits = weights_own * (dw_own - jnp.sum(weights_own * dw_own, axis=1, keepdims=True))
        d_logits = d_logits.astype(BF)
        d_norm2 = back[:, :width] + jnp.dot(d_logits, router.T, preferred_element_type=F32)
        d_resid_norm, grad_ffn_gain = jax.vjp(rms_scale, residual, ffn_gain)[1](d_norm2)
        d_resid = own(cotangent).astype(F32) + d_resid_norm
        pad = back.shape[1] - width - experts
        sent = jnp.concatenate(
            [d_resid.astype(BF), d_logits, jnp.zeros((own_rows, pad), BF)], axis=1
        )
        sent_all = gather_tokens(sent)
        d_resid_all = sent_all[:, :width]
        grad_router = lax.dot_general(
            normed_all,
            sent_all[:, width : width + experts],
            (((0,), (0,)), ((), ())),
            preferred_element_type=F32,
        )
        d_resid_bf = jnp.concatenate(split_relative(d_resid_all[:row_count]), axis=0)
        grad_out = lax.dot_general(
            attn_all, d_resid_all, (((0,), (0,)), ((), ())), preferred_element_type=F32
        )

        d_attn = jnp.dot(d_resid_bf, w_out.T, preferred_element_type=F32).astype(BF)
        d_qrot, d_krot, d_vals = attend_back(
            query_rot, key_rot, value_rot, segments, lse, d_attn, kv_here, head_dim
        )
        prep = lambda raw_in, gain_in: head_prep(raw_in, gain_in, cosine_table, sine_table)
        d_qraw, grad_qgain = jax.vjp(prep, query_raw, q_gain)[1](d_qrot)
        d_kraw, grad_kgain = jax.vjp(prep, key_raw, k_gain)[1](d_krot)
        d_qkv = jnp.concatenate([d_qraw.astype(BF), d_kraw.astype(BF), d_vals.astype(BF)], axis=1)
        d_qkv_all = gather_batches(jnp.concatenate(split_relative(d_qkv), axis=0))
        q_width = w_query.shape[1]
        k_width = w_key.shape[1]
        input_all, _ = lax.optimization_barrier((own(layer_input), normed_all))
        normed1_all = rms_scale(gather_tokens(input_all).astype(F32), attn_gain).astype(BF)

        def over_tokens(grads):
            return lax.dot_general(
                normed1_all, grads, (((0,), (0,)), ((), ())), preferred_element_type=F32
            )

        grad_query = over_tokens(d_qkv_all[:, :q_width])
        grad_key = over_tokens(d_qkv_all[:, q_width : q_width + k_width])
        grad_value = over_tokens(d_qkv_all[:, q_width + k_width :])
        d_norm1 = jnp.dot(d_qkv[:, :q_width], w_query.T, preferred_element_type=F32)
        d_norm1 = d_norm1 + jnp.dot(
            d_qkv[:, q_width : q_width + k_width], w_key.T, preferred_element_type=F32
        )
        d_norm1 = d_norm1 + jnp.dot(
            d_qkv[:, q_width + k_width :], w_value.T, preferred_element_type=F32
        )
        grad_attn_gain = jax.vjp(lambda gain: rms_scale(x_float, gain), attn_gain)[1](d_norm1)[0]
        d_norm1_own = reduce_tensor(split_relative(d_norm1.astype(BF)), BF, F32)
        d_x_norm = jax.vjp(lambda rows: rms_scale(rows, attn_gain), x_own)[1](d_norm1_own)[0]
        d_input = (d_resid + d_x_norm).astype(BF)
        d_input = jnp.concatenate(relative(over_tensor(d_input)), axis=0).astype(F32)
        gains = jnp.concatenate([grad_attn_gain, grad_ffn_gain, grad_qgain, grad_kgain])
        gains = sum_all(gains.reshape(-1, 128)).reshape(-1)
        return (
            layer_out,
            d_input,
            gains[:width],
            grad_query,
            grad_key,
            grad_value,
            gains[2 * width : 2 * width + head_dim],
            gains[2 * width + head_dim :],
            grad_out,
            gains[width : 2 * width],
            grad_router,
            grad_gate,
            grad_up,
            grad_down,
        )

    return on_device


def solution(mesh):
    in_specs = (
        P("dp", None),
        P("dp", None),
        P("dp", None),
        P("dp", None),
        P(),
        P(None, "tensor"),
        P(None, "tensor"),
        P(None, "tensor"),
        P(),
        P(),
        P("tensor", None),
        P(),
        P(),
        P("dp", None, "tensor"),
        P("dp", None, "tensor"),
        P("dp", "tensor", None),
    )
    out_specs = (
        P("dp", None),
        P("dp", None),
        P(),
        P(None, "tensor"),
        P(None, "tensor"),
        P(None, "tensor"),
        P(),
        P(),
        P("tensor", None),
        P(),
        P(),
        P("dp", None, "tensor"),
        P("dp", None, "tensor"),
        P("dp", "tensor", None),
    )
    return jax.shard_map(
        make_device_fn(mesh), mesh=mesh, in_specs=in_specs, out_specs=out_specs, check_vma=False
    )
```

```python
import jax
import jax.numpy as jnp
from jax import lax
from jax.sharding import PartitionSpec as P

CAP = 40
EPSILON = 1e-06
ROPE_BASE = 1000000.0
BF = jnp.bfloat16
F32 = jnp.float32


def rms_scale(values, gain_vec):
    return (
        values * lax.rsqrt(jnp.mean(values * values, axis=-1, keepdims=True) + EPSILON) * gain_vec
    )


def seq_positions(segments):
    index = jnp.arange(segments.shape[0], dtype=jnp.int32)
    before = jnp.sum((segments[None, :] < segments[:, None]).astype(jnp.int32), axis=1)
    return index - before


def rope_tables(positions, head_dim):
    half_dim = head_dim // 2
    exponent = jnp.arange(half_dim, dtype=F32) * (2.0 / head_dim)
    frequency = jnp.exp(-exponent * jnp.log(F32(ROPE_BASE)))
    angle_table = positions.astype(F32)[:, None] * frequency[None, :]
    angle_table = jnp.concatenate([angle_table, angle_table], axis=1)
    return (jnp.cos(angle_table), jnp.sin(angle_table))


def head_prep(raw_proj, gain_vec, cosine_table, sine_table):
    row_count = raw_proj.shape[0]
    head_dim = gain_vec.shape[0]
    split_heads = rms_scale(raw_proj.reshape(row_count, -1, head_dim), gain_vec)
    half_dim = head_dim // 2
    turned = jnp.concatenate([-split_heads[..., half_dim:], split_heads[..., :half_dim]], axis=-1)
    rotated = split_heads * cosine_table[:, None, :] + turned * sine_table[:, None, :]
    return rotated.reshape(row_count, -1)


def masked_scores(query_heads, key_heads, segments):
    rows = query_heads.shape[0]
    scores = jnp.einsum("qhgd,shd->hgqs", query_heads, key_heads, preferred_element_type=F32)
    scores = scores * query_heads.shape[-1] ** (-0.5)
    index = jnp.arange(rows, dtype=jnp.int32)
    allowed = (segments[:, None] == segments[None, :]) & (index[:, None] >= index[None, :])
    return jnp.where(allowed[None, None], scores, -jnp.inf)


def attend(query_rot, key_rot, value_rot, segments, kv_count, head_dim):
    rows = query_rot.shape[0]
    query_heads = query_rot.reshape(rows, kv_count, -1, head_dim)
    key_heads = key_rot.reshape(rows, kv_count, head_dim)
    value_heads = value_rot.reshape(rows, kv_count, head_dim)
    scores = masked_scores(query_heads, key_heads, segments)
    highest = jnp.max(scores, axis=-1, keepdims=True)
    exponent = jnp.exp(scores - highest)
    denominator = jnp.sum(exponent, axis=-1, keepdims=True)
    probs_bf = (exponent / denominator).astype(BF)
    lse = highest[..., 0] + jnp.log(denominator[..., 0])
    mixed = jnp.einsum("hgqs,shd->qhgd", probs_bf, value_heads, preferred_element_type=F32)
    return (mixed.astype(BF).reshape(rows, -1), lse)


def attend_back(query_rot, key_rot, value_rot, segments, lse, grad_heads, kv_count, head_dim):
    rows = query_rot.shape[0]
    query_heads = query_rot.reshape(rows, kv_count, -1, head_dim)
    key_heads = key_rot.reshape(rows, kv_count, head_dim)
    value_heads = value_rot.reshape(rows, kv_count, head_dim)
    scores = masked_scores(query_heads, key_heads, segments)
    probs = jnp.exp(scores - lse[..., None])
    grad_block = grad_heads.reshape(rows, kv_count, -1, head_dim)
    d_values = jnp.einsum(
        "hgqs,qhgd->shd", probs.astype(BF), grad_block, preferred_element_type=F32
    )
    d_prob = jnp.einsum("qhgd,shd->hgqs", grad_block, value_heads, preferred_element_type=F32)
    row_delta = jnp.sum(probs * d_prob, axis=-1, keepdims=True)
    d_score = (probs * (d_prob - row_delta) * head_dim ** (-0.5)).astype(BF)
    d_query = jnp.einsum("hgqs,shd->qhgd", d_score, key_heads, preferred_element_type=F32)
    d_keys = jnp.einsum("hgqs,qhgd->shd", d_score, query_heads, preferred_element_type=F32)
    return (d_query.reshape(rows, -1), d_keys.reshape(rows, -1), d_values.reshape(rows, -1))


def make_device_fn(mesh):
    n_dp = mesh.shape["dp"]
    n_tp = mesh.shape["tensor"]

    def rot(x, step):
        return lax.ppermute(x, "dp", [(i, (i + step) % n_dp) for i in range(n_dp)])

    def flip(x, mask):
        return lax.ppermute(x, "tensor", [(i, i ^ mask) for i in range(n_tp)])

    groups = 2 if n_dp % 2 == 0 else 1
    per = n_dp // groups
    order = (0, 2, 1, 3)

    def tied(x, marker):
        return lax.optimization_barrier((x, marker))[0]

    def relative(quarters):
        own = lax.axis_index("tensor")
        for bit in (1, 2):
            on = (own & bit) != 0
            quarters = [jnp.where(on, quarters[q ^ bit], quarters[q]) for q in range(n_tp)]
        return quarters

    def split_relative(x):
        return relative(jnp.split(x, n_tp, axis=0))

    def over_tensor(x):
        across = flip(x, 2)
        return [x, flip(x, 1), across, flip(across, 1)]

    def gather_tokens(x):
        blocks = [x] + [rot(x, step) for step in range(1, n_dp)]
        out = []
        for g in range(groups):
            held = over_tensor(jnp.concatenate(blocks[g * per : (g + 1) * per], axis=0))
            out.extend(held[m] for m in order)
        return jnp.concatenate(out, axis=0)

    def gather_batches(x):
        rows = x[0].shape[0]
        x = jnp.concatenate(x, axis=0)
        blocks = [x] + [rot(x, step) for step in range(1, n_dp)]
        return jnp.concatenate(
            [
                blocks[g * per + s][m * rows : (m + 1) * rows]
                for g in range(groups)
                for m in order
                for s in range(per)
            ],
            axis=0,
        )

    def own_batch(x, rows):
        parts = [None] * n_tp
        for place, m in enumerate(order):
            parts[m] = x[place * per * rows : place * per * rows + rows]
        return jnp.concatenate(relative(parts), axis=0)

    def add_up(a, b, kind):
        return (a.astype(F32) + b.astype(F32)).astype(kind)

    def reduce_tensor(parts, kind, last):
        low = add_up(parts[0], flip(parts[1], 1), kind)
        high = add_up(parts[2], flip(parts[3], 1), kind)
        return add_up(low, flip(high, 2), last)

    def reduce_tokens(x, rows):
        grid = x.reshape(groups, 2, 2, per * rows, x.shape[1])
        total = None
        sums = [None] * n_dp
        first = None
        for g in reversed(range(groups)):
            pair = add_up(grid[g, 0], flip(grid[g, 1], 1), BF)
            first = pair if first is None else first
            part = add_up(pair[0], flip(pair[1], 2), BF)
            for s in range(per):
                sums[g * per + s] = part[s * rows : (s + 1) * rows]
        for step in list(range(n_dp - 1, 0, -1)) + [0]:
            part = sums[step] if step == 0 else rot(sums[step], n_dp - step)
            total = part.astype(F32) if total is None else total + part.astype(F32)
        return total, first

    def sum_all(x):
        total = x
        for step in range(1, n_dp):
            total = total + rot(x, step)
        return sum(over_tensor(total)[1:], total)

    def on_device(
        layer_input,
        cotangent,
        segment_ids,
        routes,
        attn_gain,
        w_query,
        w_key,
        w_value,
        q_gain,
        k_gain,
        w_out,
        ffn_gain,
        router,
        w_gate,
        w_up,
        w_down,
    ):
        segments = segment_ids[0]
        row_count, width = layer_input.shape
        own_rows = row_count // n_tp
        head_dim = q_gain.shape[0]
        kv_here = w_key.shape[1] // head_dim
        experts_here = w_gate.shape[0]
        experts = router.shape[1]
        tokens = n_dp * row_count
        slots = n_dp * CAP
        tensor_at = lax.axis_index("tensor")
        first_expert = lax.axis_index("dp") * experts_here
        first_row = tensor_at * own_rows

        def own(x):
            return lax.dynamic_slice_in_dim(x, first_row, own_rows, axis=0)

        route_rows = jnp.concatenate(split_relative(routes), axis=0).T
        route_rows = [route_rows] + [rot(route_rows, step) for step in range(1, n_dp)]
        route_rows = jnp.stack(route_rows).reshape(groups, per, -1, n_tp, own_rows)
        route_rows = route_rows[:, :, :, jnp.array(order)]
        routes_all = jnp.transpose(route_rows, (0, 3, 1, 4, 2)).reshape(tokens, -1)
        cot_all = gather_tokens(own(cotangent))

        cosine_table, sine_table = rope_tables(seq_positions(segments), head_dim)
        x_float = layer_input.astype(F32)
        normed1 = rms_scale(x_float, attn_gain).astype(BF)
        query_raw = jnp.dot(normed1, w_query, preferred_element_type=F32)
        key_raw = jnp.dot(normed1, w_key, preferred_element_type=F32)
        value_rot = jnp.dot(normed1, w_value, preferred_element_type=F32).astype(BF)
        query_rot = head_prep(query_raw, q_gain, cosine_table, sine_table).astype(BF)
        key_rot = head_prep(key_raw, k_gain, cosine_table, sine_table).astype(BF)
        attn_mixed, lse = attend(query_rot, key_rot, value_rot, segments, kv_here, head_dim)
        partial_attn = jnp.dot(attn_mixed, w_out, preferred_element_type=F32)
        x_own = own(layer_input).astype(F32)
        residual = x_own + reduce_tensor(split_relative(partial_attn), F32, F32)
        normed2 = rms_scale(residual, ffn_gain).astype(BF)

        normed_all = gather_tokens(normed2)
        later = tied((own(layer_input), tuple(split_relative(attn_mixed))), normed_all)
        attn_all = gather_batches(list(later[1]))

        def dense_weights(rows, chosen):
            logits = jnp.dot(rows, router, preferred_element_type=F32)
            marks = jnp.any(
                chosen[:, :, None] == jnp.arange(experts, dtype=jnp.int32)[None, None, :], axis=1
            )
            shown = jnp.where(marks, logits, -jnp.inf)
            power = jnp.exp(shown - jnp.max(shown, axis=-1, keepdims=True))
            return power / jnp.sum(power, axis=-1, keepdims=True)

        weights_all = dense_weights(normed_all, routes_all)
        weights_here = lax.dynamic_slice_in_dim(weights_all.T, first_expert, experts_here, axis=0)
        names = first_expert + jnp.arange(experts_here, dtype=jnp.int32)
        marks = jnp.any(routes_all.T[None] == names[:, None, None], axis=1)
        index = jnp.arange(row_count, dtype=jnp.int32)
        earlier = (index[:, None] < index[None, :]).astype(BF)
        grouped = marks.astype(BF).reshape(experts_here, n_dp, row_count)
        place = jnp.einsum("ebt,tu->ebu", grouped, earlier, preferred_element_type=F32)
        counts = jnp.sum(grouped.astype(F32), axis=2)
        batch_at = jnp.arange(n_dp)
        begins = jnp.sum(
            jnp.where(batch_at[:, None] > batch_at[None, :], counts[:, None, :], 0.0), axis=2
        )
        place = (place + begins[:, :, None]).astype(jnp.int32).reshape(experts_here, tokens)
        place = jnp.where(marks, place, -1)
        picks = place[:, None, :] == jnp.arange(slots, dtype=jnp.int32)[None, :, None]
        one_hot = picks.astype(BF).reshape(experts_here * slots, tokens)

        def to_slots(rows):
            packed = jnp.dot(one_hot, rows, preferred_element_type=F32).astype(BF)
            return packed.reshape(experts_here, slots, width)

        def to_tokens(packed):
            packed = packed.reshape(experts_here * slots, width)
            return lax.dot_general(
                one_hot, packed, (((0,), (0,)), ((), ())), preferred_element_type=F32
            ).astype(BF)

        slot_weight = jnp.sum(jnp.where(picks, weights_here[:, None, :], 0.0), axis=2)

        cot_in = to_slots(cot_all)
        raw_act = jnp.einsum("erd,efd->erf", cot_in, w_down, preferred_element_type=F32)
        normed_all, raw_act = lax.optimization_barrier((normed_all, raw_act))
        expert_in = to_slots(normed_all)
        gate_pre = jnp.einsum("erd,edf->erf", expert_in, w_gate, preferred_element_type=F32)
        up_pre = jnp.einsum("erd,edf->erf", expert_in, w_up, preferred_element_type=F32)
        sigmoid_g = jax.nn.sigmoid(gate_pre)
        silu_g = gate_pre * sigmoid_g
        activation = (silu_g * up_pre).astype(BF).astype(F32)
        slot_dw = jnp.sum(activation * raw_act, axis=2)
        weighted = (activation * slot_weight[:, :, None]).astype(BF)
        d_act = raw_act * slot_weight[:, :, None]
        d_gate = (d_act * up_pre * sigmoid_g * (1.0 + gate_pre * (1.0 - sigmoid_g))).astype(BF)
        d_up = (d_act * silu_g).astype(BF)
        d_in = jnp.einsum("erf,edf->erd", d_gate, w_gate, preferred_element_type=F32)
        d_in = (
            d_in + jnp.einsum("erf,edf->erd", d_up, w_up, preferred_element_type=F32)
        ).astype(BF)
        d_weights = jnp.sum(jnp.where(picks, slot_dw[:, :, None], 0.0), axis=1)
        d_weights = lax.dynamic_update_slice(
            jnp.zeros((-(-experts // 128) * 128, tokens), F32), d_weights, (first_expert, 0)
        )
        back = jnp.concatenate([to_tokens(d_in), d_weights.T.astype(BF)], axis=1)
        back, marker = reduce_tokens(back, own_rows)

        expert_in, d_gate, d_up, weighted = tied((expert_in, d_gate, d_up, weighted), marker)
        expert_out = jnp.einsum(
            "erf,efd->erd", weighted, w_down, preferred_element_type=F32
        ).astype(BF)
        moe_terms = to_tokens(expert_out)
        grad_gate = jnp.einsum("erd,erf->edf", expert_in, d_gate, preferred_element_type=F32)
        grad_up = jnp.einsum("erd,erf->edf", expert_in, d_up, preferred_element_type=F32)

        weights_own = dense_weights(normed2, own(routes))
        dw_own = back[:, width : width + experts]
        d_logits = weights_own * (dw_own - jnp.sum(weights_own * dw_own, axis=1, keepdims=True))
        d_logits = d_logits.astype(BF)
        d_norm2 = back[:, :width] + jnp.dot(d_logits, router.T, preferred_element_type=F32)
        d_resid_norm, grad_ffn_gain = jax.vjp(rms_scale, residual, ffn_gain)[1](d_norm2)
        d_resid = own(cotangent).astype(F32) + d_resid_norm
        pad = back.shape[1] - width - experts
        sent = jnp.concatenate(
            [d_resid.astype(BF), d_logits, jnp.zeros((own_rows, pad), BF)], axis=1
        )
        sent_all = gather_tokens(sent)
        weighted, cot_in = tied((weighted, cot_in), sent)
        grad_down = jnp.einsum("erf,erd->efd", weighted, cot_in, preferred_element_type=F32)
        moe = reduce_tokens(tied(moe_terms, sent_all), own_rows)[0]
        layer_out = (residual + moe).astype(BF)
        layer_out = jnp.concatenate(relative(over_tensor(layer_out)), axis=0)
        d_resid_all = sent_all[:, :width]
        grad_router = lax.dot_general(
            normed_all,
            sent_all[:, width : width + experts],
            (((0,), (0,)), ((), ())),
            preferred_element_type=F32,
        )
        d_resid_bf = own_batch(d_resid_all, own_rows)
        grad_out = lax.dot_general(
            attn_all, d_resid_all, (((0,), (0,)), ((), ())), preferred_element_type=F32
        )

        d_attn = jnp.dot(d_resid_bf, w_out.T, preferred_element_type=F32).astype(BF)
        d_qrot, d_krot, d_vals = attend_back(
            query_rot, key_rot, value_rot, segments, lse, d_attn, kv_here, head_dim
        )
        prep = lambda raw_in, gain_in: head_prep(raw_in, gain_in, cosine_table, sine_table)
        d_qraw, grad_qgain = jax.vjp(prep, query_raw, q_gain)[1](d_qrot)
        d_kraw, grad_kgain = jax.vjp(prep, key_raw, k_gain)[1](d_krot)
        d_qkv = jnp.concatenate([d_qraw.astype(BF), d_kraw.astype(BF), d_vals.astype(BF)], axis=1)
        d_qkv_all = gather_batches(split_relative(d_qkv))
        q_width = w_query.shape[1]
        k_width = w_key.shape[1]
        normed1_all = rms_scale(gather_tokens(later[0]).astype(F32), attn_gain).astype(BF)

        def over_tokens(grads):
            return lax.dot_general(
                normed1_all, grads, (((0,), (0,)), ((), ())), preferred_element_type=F32
            )

        grad_query = over_tokens(d_qkv_all[:, :q_width])
        grad_key = over_tokens(d_qkv_all[:, q_width : q_width + k_width])
        grad_value = over_tokens(d_qkv_all[:, q_width + k_width :])
        d_norm1 = jnp.dot(d_qkv[:, :q_width], w_query.T, preferred_element_type=F32)
        d_norm1 = d_norm1 + jnp.dot(
            d_qkv[:, q_width : q_width + k_width], w_key.T, preferred_element_type=F32
        )
        d_norm1 = d_norm1 + jnp.dot(
            d_qkv[:, q_width + k_width :], w_value.T, preferred_element_type=F32
        )
        grad_attn_gain = jax.vjp(lambda gain: rms_scale(x_float, gain), attn_gain)[1](d_norm1)[0]
        d_norm1_own = reduce_tensor(split_relative(d_norm1.astype(BF)), BF, F32)
        d_x_norm = jax.vjp(lambda rows: rms_scale(rows, attn_gain), x_own)[1](d_norm1_own)[0]
        d_input = (d_resid + d_x_norm).astype(BF)
        d_input = jnp.concatenate(relative(over_tensor(d_input)), axis=0).astype(F32)
        gains = jnp.concatenate([grad_attn_gain, grad_ffn_gain, grad_qgain, grad_kgain])
        gains = sum_all(gains.reshape(-1, 128)).reshape(-1)
        return (
            layer_out,
            d_input,
            gains[:width],
            grad_query,
            grad_key,
            grad_value,
            gains[2 * width : 2 * width + head_dim],
            gains[2 * width + head_dim :],
            grad_out,
            gains[width : 2 * width],
            grad_router,
            grad_gate,
            grad_up,
            grad_down,
        )

    return on_device


def solution(mesh):
    in_specs = (
        P("dp", None),
        P("dp", None),
        P("dp", None),
        P("dp", None),
        P(),
        P(None, "tensor"),
        P(None, "tensor"),
        P(None, "tensor"),
        P(),
        P(),
        P("tensor", None),
        P(),
        P(),
        P("dp", None, "tensor"),
        P("dp", None, "tensor"),
        P("dp", "tensor", None),
    )
    out_specs = (
        P("dp", None),
        P("dp", None),
        P(),
        P(None, "tensor"),
        P(None, "tensor"),
        P(None, "tensor"),
        P(),
        P(),
        P("tensor", None),
        P(),
        P(),
        P("dp", None, "tensor"),
        P("dp", None, "tensor"),
        P("dp", "tensor", None),
    )
    return jax.shard_map(
        make_device_fn(mesh), mesh=mesh, in_specs=in_specs, out_specs=out_specs, check_vma=False
    )
```
